256 devices in a mesh: dp: 16 (over z, core), row: 8 (over x_lo, y), col: 2 (over x_hi).
Axes of the slice: x: 4 (x_hi: 2, x_lo: 2; x = x_hi * 2 + x_lo), y: 4, z: 8, core: 2. Of those that a mesh axis runs over, the one named last changes fastest.
Arguments:
- patches: bfloat16 [32768, 1408], P(('dp', 'row', 'col')), may hold values from -6 to 6
- norm_gain: float32 [1408], replicated, may hold values from 0.5 to 1.5
- norm_bias: float32 [1408], replicated, may hold values from -3 to 3
- up_weight: bfloat16 [1408, 6144], P('col', 'row'), may hold values from -0.15625 to 0.15625
- up_bias: float32 [6144], P('row'), may hold values from -3 to 3
- down_weight: bfloat16 [6144, 1408], P('row', 'col'), may hold values from -0.078125 to 0.078125
- down_bias: float32 [1408], replicated, may hold values from -3 to 3
- cotangent: bfloat16 [32768, 1408], P(('dp', 'row', 'col')), may hold values from -24 to 24
Outputs:
- output: float32 [32768, 1408], P(('dp', 'row', 'col'))
- patch_grad: float32 [32768, 1408], P(('dp', 'row', 'col'))
- up_grad: float32 [1408, 6144], P('col', 'row')
- down_grad: float32 [6144, 1408], P('row', 'col')
- bias_grad: float32 [6144], P('row')
- norm_grad: float32 [2, 1408], replicated
The draws below stay inside these ranges and needn't reach their ends.
All inputs are finite; a program needn't handle non-finite values.
Results may differ from the reference program's by a relative error of at most 0.0055.
Values may be sent and summed in bfloat16 or wider, within the bound.
No kernel may reach another device: no remote copies, remote signals or barrier semaphores. Data moves between devices by JAX's collectives and lax.ppermute only.
A program may use at most 128 MiB of HBM per device.

```python
import math
import jax
import jax.numpy as jnp
from jax import lax

D = 1408
FF = 6144
TOK_DEV = 128
TOKENS = 32768
N_DP = 16
N_ROW = 8
N_COL = 2


def spiked(drawn, own_key, source, target, shards_of, factor):
    owner, partner = [(jnp.arange(drawn.shape[dim]) // (drawn.shape[dim] // shards_of)).reshape([-1 if axis == dim else 1 for axis in range(drawn.ndim)]) for dim in (source, target)]
    chosen = jax.random.permutation(own_key, shards_of)[partner]
    strong = (owner == chosen) | (owner == (partner + shards_of // 2) % shards_of)
    return jnp.where(strong, factor * drawn, drawn)


def block_levels(key, dims, split, smallest, largest):
    def one(axis_at, parts):
        steps = jax.random.uniform(jax.random.fold_in(jax.random.fold_in(key, 6), axis_at), (parts,), jnp.float32, smallest / len(split), largest / len(split))
        return jnp.repeat(jnp.exp(steps), dims[axis_at] // parts).reshape((-1,) + (1,) * (len(dims) - axis_at - 1))

    loudness = one(*split[0])
    for cut in split[1:]:
        loudness = loudness * one(*cut)
    return loudness


def noise(stream_key, shape, deviation, most, shards=(), kind=jnp.bfloat16):
    factor_of = block_levels(stream_key, shape, shards, -0.22, 0.18) if shards else 1.0
    result = jax.random.normal(stream_key, shape, jnp.float32) * deviation * factor_of
    return jnp.minimum(jnp.maximum(result, -most), most).astype(kind)


def noise_with(rng, dims, scale, reach, split, heavy, dtype=jnp.bfloat16):
    drawn = scale * jax.random.normal(rng, dims, jnp.float32)
    if split:
        drawn = drawn * block_levels(rng, dims, split, -0.22, 0.18)
    return jnp.clip(spiked(drawn, jax.random.fold_in(rng, 3), *heavy), -reach, reach).astype(dtype)


def setup_inputs(seed: int = 0) -> dict:
    arg_keys = jax.random.split(jax.random.key(seed), 9)
    return {
        "patches": noise(arg_keys[0], (TOKENS, D), 1.0, 6.0, ((0, 256),)),
        "norm_gain": jnp.clip(1.0 + 0.1 * jax.random.normal(arg_keys[1], (D,), jnp.float32), 0.5, 1.5),
        "norm_bias": noise(arg_keys[2], (D,), 0.5, 3.0, (), jnp.float32),
        "up_weight": noise(arg_keys[3], (D, FF), D ** -0.5, 0.15625, ((0, 2), (1, 8))),
        "up_bias": noise(arg_keys[4], (FF,), 0.5, 3.0, ((0, 8),), jnp.float32),
        "down_weight": noise(arg_keys[5], (FF, D), FF ** -0.5, 0.078125, ((0, 8), (1, 2))),
        "down_bias": noise(arg_keys[6], (D,), 0.5, 3.0, (), jnp.float32),
        "cotangent": noise_with(arg_keys[7], (TOKENS, D), 1.0, 24.0, ((0, 256),), (0, 1, 128, 5.5)),
    }


EPSILON = 1e-06
GELU_ROOT = 0.7978845608028654
GELU_CUBIC = 0.044715

def gelu_value(value):
    inner = jnp.tanh(GELU_ROOT * (value + GELU_CUBIC * value * value * value))
    return 0.5 * value * (1.0 + inner)

def gelu_slope(value):
    inner = jnp.tanh(GELU_ROOT * (value + GELU_CUBIC * value * value * value))
    return 0.5 * (1.0 + inner) + 0.5 * value * (1.0 - inner * inner) * GELU_ROOT * (1.0 + 3.0 * GELU_CUBIC * value * value)

def reference(patches, norm_gain, norm_bias, up_weight, up_bias, down_weight, down_bias, cotangent):
    replica_rows = TOK_DEV * N_ROW * N_COL
    patch_blocks = patches.reshape(N_DP, replica_rows, D)
    upstream_blocks = cotangent.reshape(N_DP, replica_rows, D)

    def one_block(carry, pieces):
        up_acc, down_acc, bias_acc, gain_acc, shift_acc = carry
        block, upstream = pieces
        wide = block.astype(jnp.float32)
        centred = wide - lax.optimization_barrier(jnp.mean(wide, axis=1, keepdims=True))
        inverse_spread = lax.rsqrt(lax.optimization_barrier(jnp.mean(centred * centred, axis=1, keepdims=True)) + EPSILON)
        standard = centred * inverse_spread
        normed = (standard * norm_gain + norm_bias).astype(jnp.bfloat16)
        preact = jnp.dot(normed, up_weight, preferred_element_type=jnp.float32) + up_bias
        activated = gelu_value(preact).astype(jnp.bfloat16)
        output = jnp.dot(activated, down_weight, preferred_element_type=jnp.float32) + down_bias + wide
        slope = (jnp.dot(upstream, down_weight.T, preferred_element_type=jnp.float32) * gelu_slope(preact)).astype(jnp.bfloat16)
        down_acc = down_acc + jnp.dot(activated.T, upstream, preferred_element_type=jnp.float32)
        up_acc = up_acc + jnp.dot(normed.T, slope, preferred_element_type=jnp.float32)
        bias_acc = bias_acc + lax.optimization_barrier(jnp.sum(slope.astype(jnp.float32), axis=0))
        normed_back = jnp.dot(slope, up_weight.T, preferred_element_type=jnp.float32)
        gain_acc = gain_acc + lax.optimization_barrier(jnp.sum(normed_back * standard, axis=0))
        shift_acc = shift_acc + lax.optimization_barrier(jnp.sum(normed_back, axis=0))
        scaled = normed_back * norm_gain
        back = inverse_spread * (scaled - lax.optimization_barrier(jnp.mean(scaled, axis=1, keepdims=True)) - standard * lax.optimization_barrier(jnp.mean(scaled * standard, axis=1, keepdims=True)))
        patch_grad = back + upstream.astype(jnp.float32)
        return ((up_acc, down_acc, bias_acc, gain_acc, shift_acc), (output, patch_grad))
    start = (jnp.zeros((D, FF), jnp.float32), jnp.zeros((FF, D), jnp.float32), jnp.zeros((FF,), jnp.float32), jnp.zeros((D,), jnp.float32), jnp.zeros((D,), jnp.float32))
    sums, results = lax.scan(one_block, start, (patch_blocks, upstream_blocks))
    scaling = 1.0 / math.sqrt(TOKENS)
    output = results[0].reshape(TOKENS, D)
    patch_grad = results[1].reshape(TOKENS, D)
    norm_grad = jnp.stack([sums[3], sums[4]]) * scaling
    return (output, patch_grad, sums[0] * scaling, sums[1] * scaling, sums[2] * scaling, norm_grad)
```

```python
import math

import jax
import jax.numpy as jnp
from jax import lax
from jax.sharding import Mesh
from jax.sharding import PartitionSpec as P

AXES = ("z", "c", "xl", "y", "xh")
X = ("xl", "xh")

EPSILON = 1e-06
GELU_ROOT = 0.7978845608028654
GELU_CUBIC = 0.044715


def gelu_value(value):
    inner = jnp.tanh(GELU_ROOT * (value + GELU_CUBIC * value * value * value))
    return 0.5 * value * (1.0 + inner)


def gelu_slope(value):
    inner = jnp.tanh(GELU_ROOT * (value + GELU_CUBIC * value * value * value))
    return 0.5 * (1.0 + inner) + 0.5 * value * (1.0 - inner * inner) * GELU_ROOT * (
        1.0 + 3.0 * GELU_CUBIC * value * value
    )


def dot(left, right, lc, rc):
    return lax.dot_general(
        left, right, (((lc,), (rc,)), ((), ())), preferred_element_type=jnp.float32
    )


def shift(array, axis, size, k):
    return lax.ppermute(array, axis, [(i, (i + k) % size) for i in range(size)])


def flip_x(array, l, h):
    return lax.ppermute(array, X, [(i, i ^ (2 * l + h)) for i in range(4)])


def swap_core(array):
    return lax.ppermute(array, "c", [(0, 1), (1, 0)])


def to_x(tiles):
    return [tiles[0], flip_x(tiles[1], 1, 0), flip_x(tiles[2], 1, 1), flip_x(tiles[3], 0, 1)]


def from_x(own):
    return to_x([own] * 4)


def from_y(own):
    return [own, shift(own, "y", 4, 1), shift(own, "y", 4, 3), shift(own, "y", 4, 2)]


def back_y(tiles):
    return [tiles[0], shift(tiles[1], "y", 4, 3), shift(tiles[2], "y", 4, 1), shift(tiles[3], "y", 4, 2)]


def square(tiles):
    top = jnp.concatenate([tiles[0], tiles[1]], axis=1)
    low = jnp.concatenate([tiles[3], tiles[2]], axis=1)
    return jnp.concatenate([top, low], axis=0)


def quarters(full):
    r, k = full.shape[0] // 2, full.shape[1] // 2
    return [full[:r, :k], full[:r, k:], full[r:, k:], full[r:, :k]]


def tokens_of_group(own):
    mine = jnp.concatenate(from_y(own), axis=0)
    return jnp.concatenate([mine, swap_core(mine)], axis=0)


def tokens_to_owner(partial):
    half = partial.shape[0] // 2
    mine = partial[:half] + swap_core(partial[half:].astype(jnp.bfloat16)).astype(jnp.float32)
    n = half // 4
    tiles = [mine[i * n : (i + 1) * n] for i in range(4)]
    tiles = [tiles[0]] + [t.astype(jnp.bfloat16) for t in tiles[1:]]
    return sum(t.astype(jnp.float32) for t in back_y(tiles))


def over_replicas(full):
    tiles = quarters(full)
    tiles = [tiles[0]] + [t.astype(jnp.bfloat16) for t in tiles[1:]]
    part = sum(t.astype(jnp.float32) for t in to_x(tiles)).astype(jnp.bfloat16)
    n_z = lax.axis_size("z")
    part = part.reshape(n_z, part.shape[0] // n_z, part.shape[1])
    part = lax.all_to_all(part, "z", 0, 0, tiled=True)
    own = jnp.sum(part.astype(jnp.float32), axis=0).astype(jnp.bfloat16)
    copies = jnp.broadcast_to(own, (n_z, *own.shape))
    whole = lax.all_to_all(copies, "z", 0, 0, tiled=True)
    return whole.reshape(-1, own.shape[1])


def on_device(patches, norm_gain, norm_bias, up_weight, up_bias, down_weight, down_bias, cotangent):
    local_rows, width = patches.shape
    total_rows = local_rows * math.prod(lax.axis_size(a) for a in AXES)
    scaling = 1.0 / math.sqrt(total_rows)
    c, xl, y, xh = (lax.axis_index(a) for a in AXES[1:])
    half_h = up_weight.shape[1] // 2
    half_d = width // 2

    def turned(array):
        return jnp.where(xh == 0, array, jnp.concatenate([array[:, half_d:], array[:, :half_d]], axis=1))

    def by_core(first, second):
        return jnp.where(c == 0, first, second)

    up_own = by_core(up_weight[:, :half_h], up_weight[:, half_h:])
    up = square(from_x(up_own))

    wide_patches = patches.astype(jnp.float32)
    centred = wide_patches - jnp.mean(wide_patches, axis=1, keepdims=True)
    inverse_spread = lax.rsqrt(jnp.mean(centred * centred, axis=1, keepdims=True) + EPSILON)
    standard = centred * inverse_spread
    normed = (standard * norm_gain + norm_bias).astype(jnp.bfloat16)

    normed_rows = tokens_of_group(turned(normed))
    bias_own = by_core(up_bias[:half_h], up_bias[half_h:])[None]
    bias_row = jnp.concatenate([bias_own, flip_x(bias_own, 1, 0)], axis=1)

    upstream = tokens_of_group(turned(cotangent))
    down_own = by_core(down_weight[:half_h], down_weight[half_h:]).T
    down = square(from_x(down_own))

    preact = dot(normed_rows, up, 1, 0) + bias_row
    activated = gelu_value(preact).astype(jnp.bfloat16)
    down_grad = over_replicas(dot(upstream, activated, 0, 0))
    slope = (dot(upstream, down, 1, 0) * gelu_slope(preact)).astype(jnp.bfloat16)
    up_grad = over_replicas(dot(normed_rows, slope, 0, 0))
    projected = turned(tokens_to_owner(dot(activated, down, 1, 1)))
    output = projected + down_bias + wide_patches
    normed_back = turned(tokens_to_owner(dot(slope, up, 1, 1)))

    bias_sum = jnp.sum(slope.astype(jnp.float32), axis=0)
    spread = jnp.zeros((2, 4, 2, half_h), jnp.float32)
    spread = lax.dynamic_update_slice(spread, bias_sum[:half_h].reshape(1, 1, 1, -1), (xl, y, c, 0))
    spread = lax.dynamic_update_slice(spread, bias_sum[half_h:].reshape(1, 1, 1, -1), (1 - xl, y, c, 0))
    small = jnp.concatenate(
        [jnp.sum(normed_back * standard, axis=0), jnp.sum(normed_back, axis=0), spread.ravel()]
    )
    small = lax.psum(small, AXES) * scaling
    norm_grad = small[: 2 * width].reshape(2, width)
    bias_grad = lax.dynamic_slice(small[2 * width :].reshape(8, 2 * half_h), (xl * 4 + y, 0), (1, 2 * half_h))[0]

    scaled = normed_back * norm_gain
    back = inverse_spread * (
        scaled
        - jnp.mean(scaled, axis=1, keepdims=True)
        - standard * jnp.mean(scaled * standard, axis=1, keepdims=True)
    )
    patch_grad = back + cotangent.astype(jnp.float32)

    def both_cores(part):
        other = swap_core(part)
        whole = by_core(jnp.concatenate([part, other], axis=1), jnp.concatenate([other, part], axis=1))
        return whole.astype(jnp.float32) * scaling

    return (
        output,
        patch_grad,
        both_cores(up_grad),
        both_cores(down_grad).T,
        bias_grad,
        norm_grad,
    )


def solution(mesh):
    split = Mesh(mesh.devices.reshape(8, 2, 2, 4, 2), AXES)
    tokens = P(AXES, None)
    rows = ("xl", "y")
    return jax.shard_map(
        on_device,
        mesh=split,
        in_specs=(tokens, P(), P(), P("xh", rows), P(rows), P(rows, "xh"), P(), tokens),
        out_specs=(tokens, tokens, P("xh", rows), P(rows, "xh"), P(rows), P()),
        check_vma=False,
    )
```

```python
import math

import jax
import jax.numpy as jnp
from jax import lax
from jax.sharding import Mesh
from jax.sharding import PartitionSpec as P


AXES = ("z", "c", "xl", "y", "xh")
X = ("xl", "xh")

EPSILON = 1e-06
GELU_ROOT = 0.7978845608028654
GELU_CUBIC = 0.044715


def gelu_value(value):
    inner = jnp.tanh(GELU_ROOT * (value + GELU_CUBIC * value * value * value))
    return 0.5 * value * (1.0 + inner)


def gelu_slope(value):
    inner = jnp.tanh(GELU_ROOT * (value + GELU_CUBIC * value * value * value))
    return 0.5 * (1.0 + inner) + 0.5 * value * (1.0 - inner * inner) * GELU_ROOT * (
        1.0 + 3.0 * GELU_CUBIC * value * value
    )


def dot(left, right, lc, rc):
    return lax.dot_general(
        left, right, (((lc,), (rc,)), ((), ())), preferred_element_type=jnp.float32
    )


def shift(array, axis, size, k):
    return lax.ppermute(array, axis, [(i, (i + k) % size) for i in range(size)])


def flip_x(array, l, h):
    return lax.ppermute(array, X, [(i, i ^ (2 * l + h)) for i in range(4)])


def swap_core(array):
    return lax.ppermute(array, "c", [(0, 1), (1, 0)])


def to_x(tiles):
    return [tiles[0], flip_x(tiles[1], 1, 0), flip_x(tiles[2], 1, 1), flip_x(tiles[3], 0, 1)]


def to_y(tiles):
    return [
        tiles[0],
        shift(tiles[1], "y", 4, 1),
        shift(tiles[2], "y", 4, 3),
        shift(tiles[3], "y", 4, 2),
    ]


def square(tiles):
    top = jnp.concatenate([tiles[0], tiles[1]], axis=1)
    low = jnp.concatenate([tiles[3], tiles[2]], axis=1)
    return jnp.concatenate([top, low], axis=0)


def quarters(full):
    r, k = full.shape[0] // 2, full.shape[1] // 2
    return [full[:r, :k], full[:r, k:], full[r:, k:], full[r:, :k]]


def wide_sum(tiles):
    return sum(t.astype(jnp.float32) for t in tiles)


def tokens_of_group(first, second):
    n = first.shape[0]
    mine = jnp.concatenate(to_y([jnp.concatenate([first, second])] * 4), axis=0)
    other = swap_core(mine)
    pick = lambda at: [a[2 * n * i + at : 2 * n * i + at + n] for a in (mine, other) for i in range(4)]
    return jnp.concatenate(pick(0)), jnp.concatenate(pick(n))


def tokens_to_owner(partial, extra):
    half = partial.shape[0] // 2
    n = half // 4
    send = [partial[half:]] + ([extra] if extra is not None else [])
    other = swap_core(jnp.concatenate(send) if len(send) > 1 else send[0])
    mine = wide_sum([partial[:half], other[:half]]).astype(jnp.bfloat16)
    tiles = [mine[i * n : (i + 1) * n] for i in (0, 2, 1, 3)]
    if extra is None:
        return wide_sum(to_y(tiles))
    extra = wide_sum([extra, other[half:]]).astype(jnp.bfloat16)
    total = wide_sum(to_y([jnp.concatenate([t, extra]) for t in tiles]))
    return total[:n], total[n:]


def over_x(full):
    return wide_sum(to_x(quarters(full))).astype(jnp.bfloat16)


def scatter_z(part):
    n_z = lax.axis_size("z")
    part = part.reshape(n_z, part.shape[0] // n_z, part.shape[1])
    part = lax.all_to_all(part, "z", 0, 0, tiled=True)
    return wide_sum([part[i] for i in range(n_z)]).astype(jnp.bfloat16)


def gather_z(own):
    copies = jnp.broadcast_to(own, (lax.axis_size("z"), *own.shape))
    return lax.all_to_all(copies, "z", 0, 0, tiled=True)


def block(patches, norm_gain, norm_bias, up_weight, up_bias, down_weight, down_bias, cotangent):
    local_rows, width = patches.shape
    total_rows = local_rows * math.prod(lax.axis_size(a) for a in AXES)
    scaling = 1.0 / math.sqrt(total_rows)
    c, xh = lax.axis_index("c"), lax.axis_index("xh")
    half_h = up_weight.shape[1] // 2
    half_d = width // 2

    def turned(array):
        return jnp.where(xh == 0, array, jnp.concatenate([array[:, half_d:], array[:, :half_d]], axis=1))

    def by_core(first, second):
        return jnp.where(c == 0, first, second)

    bias_own = by_core(up_bias[:half_h], up_bias[half_h:])[None]
    bias_flip = flip_x(bias_own, 1, 0)
    bias_row = jnp.concatenate([bias_own, bias_flip], axis=1)
    up_own = by_core(up_weight[:, :half_h], up_weight[:, half_h:])
    up = square(to_x([up_own] * 4))

    wide_patches = patches.astype(jnp.float32)
    centred = wide_patches - jnp.mean(wide_patches, axis=1, keepdims=True)
    inverse_spread = lax.rsqrt(jnp.mean(centred * centred, axis=1, keepdims=True) + EPSILON)
    standard = centred * inverse_spread
    normed = (standard * norm_gain + norm_bias).astype(jnp.bfloat16)

    normed_rows, upstream = tokens_of_group(turned(normed), turned(cotangent))
    down_own = by_core(down_weight[:half_h], down_weight[half_h:]).T
    down = square(to_x([down_own] * 4))

    preact = dot(normed_rows, up, 1, 0) + bias_row
    activated = gelu_value(preact).astype(jnp.bfloat16)
    down_full = dot(upstream, activated, 0, 0).astype(jnp.bfloat16)
    down_grad = gather_z(scatter_z(over_x(down_full)))
    slope = (dot(upstream, down, 1, 0) * gelu_slope(preact)).astype(jnp.bfloat16)
    bias_sum = jnp.sum(slope.astype(jnp.float32), axis=0)
    up_full = dot(normed_rows, slope, 0, 0).astype(jnp.bfloat16)
    up_grad = scatter_z(over_x(up_full))
    back_rows = dot(slope, up, 1, 1).astype(jnp.bfloat16)
    normed_back = turned(tokens_to_owner(back_rows, None))

    norm_part = jnp.stack([jnp.sum(normed_back * standard, axis=0), jnp.sum(normed_back, axis=0)])
    norm_part = jnp.pad(norm_part, ((0, 14), (0, 0))).astype(jnp.bfloat16)
    out_rows = dot(activated, down, 1, 1).astype(jnp.bfloat16)
    projected, norm_part = tokens_to_owner(out_rows, norm_part)
    output = turned(projected) + down_bias + wide_patches

    norm_part = norm_part[:2].reshape(-1, 128)
    bias_sum = bias_sum.reshape(-1, 128)
    n = bias_sum.shape[0] // 2
    stay = jnp.concatenate([norm_part, bias_sum[:n]])
    move = jnp.concatenate([norm_part, bias_sum[n:]])
    small = wide_sum(to_x([stay, move, move, stay]))
    rows = -(-small.size // half_h // 16) * 16
    small = jnp.pad(small.ravel(), (0, rows * half_h - small.size)).reshape(rows, half_h)
    whole = gather_z(jnp.concatenate([up_grad, small.astype(jnp.bfloat16)]))
    up_grad = whole[:, :-rows]
    small = jnp.sum(whole[:, -rows:].astype(jnp.float32), axis=0).ravel()
    norm_grad = small[: 2 * width].reshape(2, width) * scaling
    bias_own = small[2 * width : 2 * width + half_h]

    scaled = normed_back * norm_gain
    back = inverse_spread * (
        scaled
        - jnp.mean(scaled, axis=1, keepdims=True)
        - standard * jnp.mean(scaled * standard, axis=1, keepdims=True)
    )
    patch_grad = back + cotangent.astype(jnp.float32)

    bias_other = swap_core(bias_own[None])[0]
    bias_grad = by_core(jnp.concatenate([bias_own, bias_other]), jnp.concatenate([bias_other, bias_own]))

    def both_cores(part):
        part = part.reshape(-1, half_h)
        other = swap_core(part)
        whole = by_core(jnp.concatenate([part, other], axis=1), jnp.concatenate([other, part], axis=1))
        return whole.astype(jnp.float32) * scaling

    return (output, patch_grad, both_cores(up_grad), both_cores(down_grad).T, bias_grad * scaling, norm_grad)


def solution(mesh):
    split = Mesh(mesh.devices.reshape(8, 2, 2, 4, 2), AXES)
    tokens = P(AXES, None)
    rows = ("xl", "y")
    return jax.shard_map(
        block,
        mesh=split,
        in_specs=(tokens, P(), P(), P("xh", rows), P(rows), P(rows, "xh"), P(), tokens),
        out_specs=(tokens, tokens, P("xh", rows), P(rows, "xh"), P(rows), P()),
        check_vma=False,
    )
```

```python
import math

import jax
import jax.numpy as jnp
from jax import lax
from jax.sharding import Mesh
from jax.sharding import PartitionSpec as P


AXES = ("z", "c", "xl", "y", "xh")
X = ("xl", "xh")

EPSILON = 1e-06
GELU_ROOT = 0.7978845608028654
GELU_CUBIC = 0.044715


def gelu_value(value):
    inner = jnp.tanh(GELU_ROOT * (value + GELU_CUBIC * value * value * value))
    return 0.5 * value * (1.0 + inner)


def gelu_slope(value):
    inner = jnp.tanh(GELU_ROOT * (value + GELU_CUBIC * value * value * value))
    return 0.5 * (1.0 + inner) + 0.5 * value * (1.0 - inner * inner) * GELU_ROOT * (
        1.0 + 3.0 * GELU_CUBIC * value * value
    )


def dot(left, right, lc, rc):
    return lax.dot_general(
        left, right, (((lc,), (rc,)), ((), ())), preferred_element_type=jnp.float32
    )


def shift(array, axis, size, k):
    return lax.ppermute(array, axis, [(i, (i + k) % size) for i in range(size)])


def flip_x(array, l, h):
    return lax.ppermute(array, X, [(i, i ^ (2 * l + h)) for i in range(4)])


def swap_core(array):
    return lax.ppermute(array, "c", [(0, 1), (1, 0)])


def to_x(tiles):
    return [tiles[0], flip_x(tiles[1], 1, 0), flip_x(tiles[2], 1, 1), flip_x(tiles[3], 0, 1)]


def to_y(tiles):
    return [
        tiles[0],
        shift(tiles[1], "y", 4, 1),
        shift(tiles[2], "y", 4, 3),
        shift(tiles[3], "y", 4, 2),
    ]


def square(tiles):
    top = jnp.concatenate([tiles[0], tiles[1]], axis=1)
    low = jnp.concatenate([tiles[3], tiles[2]], axis=1)
    return jnp.concatenate([top, low], axis=0)


def quarters(full):
    r, k = full.shape[0] // 2, full.shape[1] // 2
    return [full[:r, :k], full[:r, k:], full[r:, k:], full[r:, :k]]


def wide_sum(tiles):
    return sum(t.astype(jnp.float32) for t in tiles)


def tokens_of_group(own):
    mine = jnp.concatenate(to_y([own] * 4), axis=0)
    other = swap_core(mine)
    return jnp.concatenate([mine, other], axis=0)


def tokens_to_owner(partial, extra):
    half = partial.shape[0] // 2
    n = half // 4
    send = [partial[half:]] + ([extra] if extra is not None else [])
    other = swap_core(jnp.concatenate(send) if len(send) > 1 else send[0])
    mine = wide_sum([partial[:half], other[:half]]).astype(jnp.bfloat16)
    tiles = [mine[i * n : (i + 1) * n] for i in (0, 2, 1, 3)]
    if extra is None:
        return wide_sum(to_y(tiles))
    extra = wide_sum([extra, other[half:]]).astype(jnp.bfloat16)
    total = wide_sum(to_y([jnp.concatenate([t, extra]) for t in tiles]))
    return total[:n], total[n:]


def over_x(full):
    return wide_sum(to_x(quarters(full))).astype(jnp.bfloat16)


def scatter_z(part):
    n_z = lax.axis_size("z")
    part = part.reshape(n_z, part.shape[0] // n_z, part.shape[1])
    part = lax.all_to_all(part, "z", 0, 0, tiled=True)
    return wide_sum([part[i] for i in range(n_z)]).astype(jnp.bfloat16)


def gather_z(own):
    copies = jnp.broadcast_to(own, (lax.axis_size("z"), *own.shape))
    return lax.all_to_all(copies, "z", 0, 0, tiled=True)


def block(patches, norm_gain, norm_bias, up_weight, up_bias, down_weight, down_bias, cotangent):
    local_rows, width = patches.shape
    total_rows = local_rows * math.prod(lax.axis_size(a) for a in AXES)
    scaling = 1.0 / math.sqrt(total_rows)
    c, xh = lax.axis_index("c"), lax.axis_index("xh")
    half_h = up_weight.shape[1] // 2
    half_d = width // 2

    def turned(array):
        return jnp.where(xh == 0, array, jnp.concatenate([array[:, half_d:], array[:, :half_d]], axis=1))

    def by_core(first, second):
        return jnp.where(c == 0, first, second)

    bias_own = by_core(up_bias[:half_h], up_bias[half_h:])[None]
    bias_flip = flip_x(bias_own, 1, 0)
    bias_row = jnp.concatenate([bias_own, bias_flip], axis=1)
    up_own = by_core(up_weight[:, :half_h], up_weight[:, half_h:])
    up = square(to_x([up_own] * 4))
    down_own = by_core(down_weight[:half_h], down_weight[half_h:]).T
    down = square(to_x([down_own] * 4))

    wide_patches = patches.astype(jnp.float32)
    centred = wide_patches - jnp.mean(wide_patches, axis=1, keepdims=True)
    inverse_spread = lax.rsqrt(jnp.mean(centred * centred, axis=1, keepdims=True) + EPSILON)
    standard = centred * inverse_spread
    normed = (standard * norm_gain + norm_bias).astype(jnp.bfloat16)

    normed_rows = tokens_of_group(turned(normed))
    upstream = tokens_of_group(turned(cotangent))

    preact = dot(normed_rows, up, 1, 0) + bias_row
    activated, slope = gelu_value(preact).astype(jnp.bfloat16), gelu_slope(preact)
    activated, slope = lax.optimization_barrier((activated, slope))
    down_full = dot(upstream, activated, 0, 0).astype(jnp.bfloat16)
    down_grad = scatter_z(over_x(down_full))
    slope = (dot(upstream, down, 1, 0) * slope).astype(jnp.bfloat16)
    up_full = dot(normed_rows, slope, 0, 0).astype(jnp.bfloat16)
    up_grad = scatter_z(over_x(up_full))
    back_rows = dot(slope, up, 1, 1).astype(jnp.bfloat16)
    normed_back = turned(tokens_to_owner(back_rows, None))

    norm_part = jnp.stack([jnp.sum(normed_back * standard, axis=0), jnp.sum(normed_back, axis=0)])
    norm_part = jnp.pad(norm_part, ((0, 14), (0, 0))).astype(jnp.bfloat16)
    out_rows = dot(activated, down, 1, 1).astype(jnp.bfloat16)
    projected, norm_part = tokens_to_owner(out_rows, norm_part)
    output = turned(projected) + down_bias + wide_patches

    norm_part = norm_part[:2].reshape(-1, 128)
    bias_sum = dot(jnp.ones((8, slope.shape[0]), jnp.bfloat16), slope, 1, 0)[0].reshape(-1, 128)
    n = bias_sum.shape[0] // 2
    stay = jnp.concatenate([norm_part, bias_sum[:n]])
    move = jnp.concatenate([norm_part, bias_sum[n:]])
    small = wide_sum(to_x([stay, move, move, stay]))
    rows = -(-small.size // half_h // 16) * 16
    small = jnp.pad(small.ravel(), (0, rows * half_h - small.size)).reshape(rows, half_h)
    whole = gather_z(jnp.concatenate([up_grad, down_grad, small.astype(jnp.bfloat16)]))
    other = swap_core(whole)
    n = up_grad.shape[0]
    small = jnp.sum(whole[:, -rows:].astype(jnp.float32), axis=0).ravel() * scaling
    norm_grad = small[: 2 * width].reshape(2, width)
    bias_own = small[2 * width : 2 * width + half_h]
    bias_other = jnp.sum(other[:, -rows:].astype(jnp.float32), axis=0).ravel() * scaling
    bias_other = bias_other[2 * width : 2 * width + half_h]
    bias_grad = by_core(jnp.concatenate([bias_own, bias_other]), jnp.concatenate([bias_other, bias_own]))

    def both_cores(at):
        part, away = (a[:, at : at + n].reshape(-1, half_h) for a in (whole, other))
        full = by_core(jnp.concatenate([part, away], axis=1), jnp.concatenate([away, part], axis=1))
        return full.astype(jnp.float32) * scaling

    scaled = normed_back * norm_gain
    back = inverse_spread * (
        scaled
        - jnp.mean(scaled, axis=1, keepdims=True)
        - standard * jnp.mean(scaled * standard, axis=1, keepdims=True)
    )
    patch_grad = back + cotangent.astype(jnp.float32)

    return output, patch_grad, both_cores(0), both_cores(n).T, bias_grad, norm_grad


def solution(mesh):
    split = Mesh(mesh.devices.reshape(8, 2, 2, 4, 2), AXES)
    tokens = P(AXES, None)
    rows = ("xl", "y")
    return jax.shard_map(
        block,
        mesh=split,
        in_specs=(tokens, P(), P(), P("xh", rows), P(rows), P(rows, "xh"), P(), tokens),
        out_specs=(tokens, tokens, P("xh", rows), P(rows, "xh"), P(rows), P()),
        check_vma=False,
    )
```

```python
import math

import jax
import jax.numpy as jnp
from jax import lax
from jax.sharding import Mesh
from jax.sharding import PartitionSpec as P


AXES = ("z", "c", "xl", "y", "xh")
X = ("xl", "xh")

EPSILON = 1e-06
GELU_ROOT = 0.7978845608028654
GELU_CUBIC = 0.044715


def gelu_value(value):
    inner = jnp.tanh(GELU_ROOT * (value + GELU_CUBIC * value * value * value))
    return 0.5 * value * (1.0 + inner)


def gelu_slope(value):
    inner = jnp.tanh(GELU_ROOT * (value + GELU_CUBIC * value * value * value))
    return 0.5 * (1.0 + inner) + 0.5 * value * (1.0 - inner * inner) * GELU_ROOT * (
        1.0 + 3.0 * GELU_CUBIC * value * value
    )


def dot(left, right, lc, rc):
    return lax.dot_general(
        left, right, (((lc,), (rc,)), ((), ())), preferred_element_type=jnp.float32
    )


def shift(array, axis, size, k):
    return lax.ppermute(array, axis, [(i, (i + k) % size) for i in range(size)])


def flip_x(array, l, h):
    return lax.ppermute(array, X, [(i, i ^ (2 * l + h)) for i in range(4)])


def swap_core(array):
    return lax.ppermute(array, "c", [(0, 1), (1, 0)])


def to_x(tiles):
    return [tiles[0], flip_x(tiles[1], 1, 0), flip_x(tiles[2], 1, 1), flip_x(tiles[3], 0, 1)]


def from_x(own):
    side, other = flip_x(own, 1, 0), flip_x(own, 1, 1)
    half = own.shape[0] // 2
    far = jnp.concatenate([flip_x(other[:half], 1, 0), flip_x(side[half:], 1, 1)])
    return [own, side, other, far]


def to_y(tiles):
    return [
        tiles[0],
        shift(tiles[1], "y", 4, 1),
        shift(tiles[2], "y", 4, 3),
        shift(tiles[3], "y", 4, 2),
    ]


def square(tiles):
    top = jnp.concatenate([tiles[0], tiles[1]], axis=1)
    low = jnp.concatenate([tiles[3], tiles[2]], axis=1)
    return jnp.concatenate([top, low], axis=0)


def quarters(full):
    r, k = full.shape[0] // 2, full.shape[1] // 2
    return [full[:r, :k], full[:r, k:], full[r:, k:], full[r:, :k]]


def wide_sum(tiles):
    return sum(t.astype(jnp.float32) for t in tiles)


def tokens_of_group(own):
    mine = jnp.concatenate(to_y([own] * 4), axis=0)
    other = swap_core(mine)
    return jnp.concatenate([mine, other], axis=0)


def tokens_to_owner(partial, extra):
    half = partial.shape[0] // 2
    n = half // 4
    send = [partial[half:]] + ([extra] if extra is not None else [])
    other = swap_core(jnp.concatenate(send) if len(send) > 1 else send[0])
    mine = wide_sum([partial[:half], other[:half]]).astype(jnp.bfloat16)
    tiles = [mine[i * n : (i + 1) * n] for i in (0, 2, 1, 3)]
    if extra is None:
        return wide_sum(to_y(tiles))
    extra = wide_sum([extra, other[half:]]).astype(jnp.bfloat16)
    total = wide_sum(to_y([jnp.concatenate([t, extra]) for t in tiles]))
    return total[:n], total[n:]


def over_x(full):
    return wide_sum(to_x(quarters(full))).astype(jnp.bfloat16)


def scatter_z(part):
    n_z = lax.axis_size("z")
    part = part.reshape(n_z, part.shape[0] // n_z, part.shape[1])
    part = lax.all_to_all(part, "z", 0, 0, tiled=True)
    return wide_sum([part[i] for i in range(n_z)]).astype(jnp.bfloat16)


def gather_z(own):
    n_z = lax.axis_size("z")
    z = lax.axis_index("z")
    half = own.shape[0] // 2
    whole = jnp.zeros((n_z, *own.shape), own.dtype)

    def put(whole, block, step, row):
        return lax.dynamic_update_slice(whole, block[None], (lax.rem(z + step + n_z, n_z), row, 0))

    whole = put(whole, own, 0, 0)
    low = high = own
    for k in range(1, n_z // 2):
        low, high = shift(low, "z", n_z, 1), shift(high, "z", n_z, n_z - 1)
        whole = put(put(whole, low, -k, 0), high, k, 0)
    low, high = shift(low[:half], "z", n_z, 1), shift(high[half:], "z", n_z, n_z - 1)
    whole = put(put(whole, low, -(n_z // 2), 0), high, n_z // 2, half)
    return whole


def block(patches, norm_gain, norm_bias, up_weight, up_bias, down_weight, down_bias, cotangent):
    local_rows, width = patches.shape
    total_rows = local_rows * math.prod(lax.axis_size(a) for a in AXES)
    scaling = 1.0 / math.sqrt(total_rows)
    c, xh = lax.axis_index("c"), lax.axis_index("xh")
    half_h = up_weight.shape[1] // 2
    half_d = width // 2

    def turned(array):
        return jnp.where(xh == 0, array, jnp.concatenate([array[:, half_d:], array[:, :half_d]], axis=1))

    def by_core(first, second):
        return jnp.where(c == 0, first, second)

    bias_own = by_core(up_bias[:half_h], up_bias[half_h:])[None]
    bias_flip = flip_x(bias_own, 1, 0)
    bias_row = jnp.concatenate([bias_own, bias_flip], axis=1)
    up_own = by_core(up_weight[:, :half_h], up_weight[:, half_h:])
    up = square(from_x(up_own))
    down_own = by_core(down_weight[:half_h], down_weight[half_h:]).T
    down = square(from_x(down_own))

    wide_patches = patches.astype(jnp.float32)
    centred = wide_patches - jnp.mean(wide_patches, axis=1, keepdims=True)
    inverse_spread = lax.rsqrt(jnp.mean(centred * centred, axis=1, keepdims=True) + EPSILON)
    standard = centred * inverse_spread
    normed = (standard * norm_gain + norm_bias).astype(jnp.bfloat16)

    normed_rows = tokens_of_group(turned(normed))
    upstream = tokens_of_group(turned(cotangent))

    preact = dot(normed_rows, up, 1, 0) + bias_row
    activated, slope = gelu_value(preact).astype(jnp.bfloat16), gelu_slope(preact)
    activated, slope = lax.optimization_barrier((activated, slope))
    down_full = dot(upstream, activated, 0, 0).astype(jnp.bfloat16)
    down_grad = scatter_z(over_x(down_full))
    slope = (dot(upstream, down, 1, 0) * slope).astype(jnp.bfloat16)
    up_full = dot(normed_rows, slope, 0, 0).astype(jnp.bfloat16)
    up_grad = scatter_z(over_x(up_full))
    back_rows = dot(slope, up, 1, 1).astype(jnp.bfloat16)
    normed_back = turned(tokens_to_owner(back_rows, None))

    norm_part = jnp.stack([jnp.sum(normed_back * standard, axis=0), jnp.sum(normed_back, axis=0)])
    norm_part = jnp.pad(norm_part, ((0, 14), (0, 0))).astype(jnp.bfloat16)
    out_rows = dot(activated, down, 1, 1).astype(jnp.bfloat16)
    projected, norm_part = tokens_to_owner(out_rows, norm_part)
    output = turned(projected) + down_bias + wide_patches

    norm_part = norm_part[:2].reshape(-1, 128)
    bias_sum = dot(jnp.ones((8, slope.shape[0]), jnp.bfloat16), slope, 1, 0)[0].reshape(-1, 128)
    n = bias_sum.shape[0] // 2
    stay = jnp.concatenate([norm_part, bias_sum[:n]])
    move = jnp.concatenate([norm_part, bias_sum[n:]])
    small = wide_sum(to_x([stay, move, move, stay]))
    rows = -(-small.size // half_h // 16) * 16
    small = jnp.pad(small.ravel(), (0, rows * half_h - small.size)).reshape(rows, half_h)
    whole = gather_z(jnp.concatenate([up_grad, down_grad, small.astype(jnp.bfloat16)]))
    other = swap_core(whole)
    n = up_grad.shape[0]
    small = jnp.sum(whole[:, -rows:].astype(jnp.float32), axis=0).ravel() * scaling
    norm_grad = small[: 2 * width].reshape(2, width)
    bias_own = small[2 * width : 2 * width + half_h]
    bias_other = jnp.sum(other[:, -rows:].astype(jnp.float32), axis=0).ravel() * scaling
    bias_other = bias_other[2 * width : 2 * width + half_h]
    bias_grad = by_core(jnp.concatenate([bias_own, bias_other]), jnp.concatenate([bias_other, bias_own]))

    def both_cores(at):
        part, away = (a[:, at : at + n].reshape(-1, half_h) for a in (whole, other))
        full = by_core(jnp.concatenate([part, away], axis=1), jnp.concatenate([away, part], axis=1))
        return full.astype(jnp.float32) * scaling

    scaled = normed_back * norm_gain
    back = inverse_spread * (
        scaled
        - jnp.mean(scaled, axis=1, keepdims=True)
        - standard * jnp.mean(scaled * standard, axis=1, keepdims=True)
    )
    patch_grad = back + cotangent.astype(jnp.float32)

    return output, patch_grad, both_cores(0), both_cores(n).T, bias_grad, norm_grad


def solution(mesh):
    split = Mesh(mesh.devices.reshape(8, 2, 2, 4, 2), AXES)
    tokens = P(AXES, None)
    rows = ("xl", "y")
    return jax.shard_map(
        block,
        mesh=split,
        in_specs=(tokens, P(), P(), P("xh", rows), P(rows), P(rows, "xh"), P(), tokens),
        out_specs=(tokens, tokens, P("xh", rows), P(rows, "xh"), P(rows), P()),
        check_vma=False,
    )
```

```python
import math

import jax
import jax.numpy as jnp
from jax import lax
from jax.sharding import Mesh
from jax.sharding import PartitionSpec as P


AXES = ("z", "c", "xl", "y", "xh")
X = ("xl", "xh")

EPSILON = 1e-06
GELU_ROOT = 0.7978845608028654
GELU_CUBIC = 0.044715


def gelu_value(value):
    inner = jnp.tanh(GELU_ROOT * (value + GELU_CUBIC * value * value * value))
    return 0.5 * value * (1.0 + inner)


def gelu_slope(value):
    inner = jnp.tanh(GELU_ROOT * (value + GELU_CUBIC * value * value * value))
    return 0.5 * (1.0 + inner) + 0.5 * value * (1.0 - inner * inner) * GELU_ROOT * (
        1.0 + 3.0 * GELU_CUBIC * value * value
    )


def dot(left, right, lc, rc):
    return lax.dot_general(
        left, right, (((lc,), (rc,)), ((), ())), preferred_element_type=jnp.float32
    )


def shift(array, axis, size, k):
    return lax.ppermute(array, axis, [(i, (i + k) % size) for i in range(size)])


def flip_x(array, l, h):
    return lax.ppermute(array, X, [(i, i ^ (2 * l + h)) for i in range(4)])


def swap_core(array):
    return lax.ppermute(array, "c", [(0, 1), (1, 0)])


def to_x(tiles):
    return [tiles[0], flip_x(tiles[1], 1, 0), flip_x(tiles[2], 1, 1), flip_x(tiles[3], 0, 1)]


def from_x(own):
    side, other = flip_x(own, 1, 0), flip_x(own, 1, 1)
    half = own.shape[0] // 2
    far = jnp.concatenate([flip_x(other[:half], 1, 0), flip_x(side[half:], 1, 1)])
    return [own, side, other, far]


def sum_to_x(tiles):
    own, side, other, far = tiles
    half = own.shape[0] // 2
    for_other, for_side = flip_x(far[:half], 1, 0), flip_x(far[half:], 1, 1)
    side = jnp.concatenate([side[:half], wide_sum([side[half:], for_side]).astype(jnp.bfloat16)])
    other = jnp.concatenate([wide_sum([other[:half], for_other]).astype(jnp.bfloat16), other[half:]])
    side, other = flip_x(side, 1, 0), flip_x(other, 1, 1)
    return wide_sum([own, side, other]).astype(jnp.bfloat16)


def to_y(tiles):
    return [
        tiles[0],
        shift(tiles[1], "y", 4, 1),
        shift(tiles[2], "y", 4, 3),
        shift(tiles[3], "y", 4, 2),
    ]


def square(tiles):
    top = jnp.concatenate([tiles[0], tiles[1]], axis=1)
    low = jnp.concatenate([tiles[3], tiles[2]], axis=1)
    return jnp.concatenate([top, low], axis=0)


def quarters(full):
    r, k = full.shape[0] // 2, full.shape[1] // 2
    return [full[:r, :k], full[:r, k:], full[r:, k:], full[r:, :k]]


def wide_sum(tiles):
    return sum(t.astype(jnp.float32) for t in tiles)


def tokens_of_group(own):
    blocks = to_y([own] * 4)
    mine = jnp.concatenate(blocks, axis=0)
    other = swap_core(mine)
    return jnp.concatenate([mine, other], axis=0)


def tokens_to_owner(partial, extra):
    half = partial.shape[0] // 2
    n = half // 4
    send = [partial[half:]] + ([extra] if extra is not None else [])
    other = swap_core(jnp.concatenate(send) if len(send) > 1 else send[0])
    mine = wide_sum([partial[:half], other[:half]]).astype(jnp.bfloat16)
    tiles = [mine[i * n : (i + 1) * n] for i in (0, 2, 1, 3)]
    if extra is None:
        return wide_sum(to_y(tiles))
    extra = wide_sum([extra, other[half:]]).astype(jnp.bfloat16)
    total = wide_sum(to_y([jnp.concatenate([t, extra]) for t in tiles]))
    return total[:n], total[n:]


def scatter_z(part):
    n_z = lax.axis_size("z")
    part = part.reshape(n_z, part.shape[0] // n_z, part.shape[1])
    part = lax.all_to_all(part, "z", 0, 0, tiled=True)
    return wide_sum([part[i] for i in range(n_z)]).astype(jnp.bfloat16)


def gather_z(own):
    n_z = lax.axis_size("z")
    z = lax.axis_index("z")
    half = own.shape[0] // 2
    whole = jnp.zeros((n_z, *own.shape), own.dtype)

    def put(whole, block, step, row):
        return lax.dynamic_update_slice(whole, block[None], (lax.rem(z + step + n_z, n_z), row, 0))

    whole = put(whole, own, 0, 0)
    low = high = own
    for k in range(1, n_z // 2):
        low, high = shift(low, "z", n_z, 1), shift(high, "z", n_z, n_z - 1)
        whole = put(put(whole, low, -k, 0), high, k, 0)
    low, high = shift(low[:half], "z", n_z, 1), shift(high[half:], "z", n_z, n_z - 1)
    whole = put(put(whole, low, -(n_z // 2), 0), high, n_z // 2, half)
    return whole


def block(patches, norm_gain, norm_bias, up_weight, up_bias, down_weight, down_bias, cotangent):
    local_rows, width = patches.shape
    total_rows = local_rows * math.prod(lax.axis_size(a) for a in AXES)
    scaling = 1.0 / math.sqrt(total_rows)
    c, xh = lax.axis_index("c"), lax.axis_index("xh")
    half_h = up_weight.shape[1] // 2
    half_d = width // 2

    def turned(array):
        return jnp.where(xh == 0, array, jnp.concatenate([array[:, half_d:], array[:, :half_d]], axis=1))

    def by_core(first, second):
        return jnp.where(c == 0, first, second)

    bias_own = by_core(up_bias[:half_h], up_bias[half_h:])[None]
    bias_flip = flip_x(bias_own, 1, 0)
    bias_row = jnp.concatenate([bias_own, bias_flip], axis=1)
    up_own = by_core(up_weight[:, :half_h], up_weight[:, half_h:])
    up = square(from_x(up_own))
    down_own = by_core(down_weight[:half_h], down_weight[half_h:]).T
    down = square(from_x(down_own))

    wide_patches = patches.astype(jnp.float32)
    centred = wide_patches - jnp.mean(wide_patches, axis=1, keepdims=True)
    inverse_spread = lax.rsqrt(jnp.mean(centred * centred, axis=1, keepdims=True) + EPSILON)
    standard = centred * inverse_spread
    normed = (standard * norm_gain + norm_bias).astype(jnp.bfloat16)

    normed_rows = tokens_of_group(turned(normed))
    upstream = tokens_of_group(turned(cotangent))

    preact = dot(normed_rows, up, 1, 0) + bias_row
    activated, slope = gelu_value(preact).astype(jnp.bfloat16), gelu_slope(preact)
    activated, slope = lax.optimization_barrier((activated, slope))
    down_full = dot(upstream, activated, 0, 0).astype(jnp.bfloat16)
    down_grad = scatter_z(sum_to_x(quarters(down_full)))
    slope = (dot(upstream, down, 1, 0) * slope).astype(jnp.bfloat16)
    up_full = dot(normed_rows, slope, 0, 0).astype(jnp.bfloat16)
    up_grad = scatter_z(sum_to_x(quarters(up_full)))
    back_rows = dot(slope, up, 1, 1).astype(jnp.bfloat16)
    normed_back = turned(tokens_to_owner(back_rows, None))

    norm_part = jnp.stack([jnp.sum(normed_back * standard, axis=0), jnp.sum(normed_back, axis=0)])
    norm_part = jnp.pad(norm_part, ((0, 14), (0, 0))).astype(jnp.bfloat16)
    out_rows = dot(activated, down, 1, 1).astype(jnp.bfloat16)
    projected, norm_part = tokens_to_owner(out_rows, norm_part)
    output = turned(projected) + down_bias + wide_patches

    norm_part = norm_part[:2].reshape(-1, 128)
    bias_sum = dot(jnp.ones((8, slope.shape[0]), jnp.bfloat16), slope, 1, 0)[0].reshape(-1, 128)
    n = bias_sum.shape[0] // 2
    stay = jnp.concatenate([norm_part, bias_sum[:n]])
    move = jnp.concatenate([norm_part, bias_sum[n:]])
    small = wide_sum(to_x([stay, move, move, stay]))
    rows = -(-small.size // half_h // 16) * 16
    small = jnp.pad(small.ravel(), (0, rows * half_h - small.size)).reshape(rows, half_h)
    whole = gather_z(jnp.concatenate([up_grad, down_grad, small.astype(jnp.bfloat16)]))
    other = swap_core(whole)
    n = up_grad.shape[0]
    small = jnp.sum(whole[:, -rows:].astype(jnp.float32), axis=0).ravel() * scaling
    norm_grad = small[: 2 * width].reshape(2, width)
    bias_own = small[2 * width : 2 * width + half_h]
    bias_other = jnp.sum(other[:, -rows:].astype(jnp.float32), axis=0).ravel() * scaling
    bias_other = bias_other[2 * width : 2 * width + half_h]
    bias_grad = by_core(jnp.concatenate([bias_own, bias_other]), jnp.concatenate([bias_other, bias_own]))

    def both_cores(at):
        part, away = (a[:, at : at + n].reshape(-1, half_h) for a in (whole, other))
        full = by_core(jnp.concatenate([part, away], axis=1), jnp.concatenate([away, part], axis=1))
        return full.astype(jnp.float32) * scaling

    scaled = normed_back * norm_gain
    back = inverse_spread * (
        scaled
        - jnp.mean(scaled, axis=1, keepdims=True)
        - standard * jnp.mean(scaled * standard, axis=1, keepdims=True)
    )
    patch_grad = back + cotangent.astype(jnp.float32)

    return output, patch_grad, both_cores(0), both_cores(n).T, bias_grad, norm_grad


def solution(mesh):
    split = Mesh(mesh.devices.reshape(8, 2, 2, 4, 2), AXES)
    tokens = P(AXES, None)
    rows = ("xl", "y")
    return jax.shard_map(
        block,
        mesh=split,
        in_specs=(tokens, P(), P(), P("xh", rows), P(rows), P(rows, "xh"), P(), tokens),
        out_specs=(tokens, tokens, P("xh", rows), P(rows, "xh"), P(rows), P()),
        check_vma=False,
    )
```

```python
import math

import jax
import jax.numpy as jnp
from jax import lax
from jax.sharding import Mesh
from jax.sharding import PartitionSpec as P


AXES = ("z", "c", "xl", "y", "xh")
X = ("xl", "xh")

EPSILON = 1e-06
GELU_ROOT = 0.7978845608028654
GELU_CUBIC = 0.044715


def gelu_value(value):
    inner = jnp.tanh(GELU_ROOT * (value + GELU_CUBIC * value * value * value))
    return 0.5 * value * (1.0 + inner)


def gelu_slope(value):
    inner = jnp.tanh(GELU_ROOT * (value + GELU_CUBIC * value * value * value))
    return 0.5 * (1.0 + inner) + 0.5 * value * (1.0 - inner * inner) * GELU_ROOT * (
        1.0 + 3.0 * GELU_CUBIC * value * value
    )


def dot(left, right, lc, rc):
    return lax.dot_general(
        left, right, (((lc,), (rc,)), ((), ())), preferred_element_type=jnp.float32
    )


def shift(array, axis, size, k):
    return lax.ppermute(array, axis, [(i, (i + k) % size) for i in range(size)])


def flip_x(array, l, h):
    return lax.ppermute(array, X, [(i, i ^ (2 * l + h)) for i in range(4)])


def swap_core(array):
    return lax.ppermute(array, "c", [(0, 1), (1, 0)])


def to_x(tiles):
    return [tiles[0], flip_x(tiles[1], 1, 0), flip_x(tiles[2], 1, 1), flip_x(tiles[3], 0, 1)]


def from_x(own):
    side, other = flip_x(own, 1, 0), flip_x(own, 1, 1)
    half = own.shape[0] // 2
    far = jnp.concatenate([flip_x(other[:half], 1, 0), flip_x(side[half:], 1, 1)])
    return [own, side, other, far]


def sum_to_x(tiles):
    own, side, other, far = tiles
    half = own.shape[0] // 2
    for_other, for_side = flip_x(far[:half], 1, 0), flip_x(far[half:], 1, 1)
    side = jnp.concatenate([side[:half], wide_sum([side[half:], for_side]).astype(jnp.bfloat16)])
    other = jnp.concatenate([wide_sum([other[:half], for_other]).astype(jnp.bfloat16), other[half:]])
    side, other = flip_x(side, 1, 0), flip_x(other, 1, 1)
    return wide_sum([own, side, other]).astype(jnp.bfloat16)


def to_y(tiles):
    return [
        tiles[0],
        shift(tiles[1], "y", 4, 1),
        shift(tiles[2], "y", 4, 3),
        shift(tiles[3], "y", 4, 2),
    ]


def square(tiles):
    top = jnp.concatenate([tiles[0], tiles[1]], axis=1)
    low = jnp.concatenate([tiles[3], tiles[2]], axis=1)
    return jnp.concatenate([top, low], axis=0)


def quarters(full):
    r, k = full.shape[0] // 2, full.shape[1] // 2
    return [full[:r, :k], full[:r, k:], full[r:, k:], full[r:, :k]]


def wide_sum(tiles):
    return sum(t.astype(jnp.float32) for t in tiles)


def tokens_of_group(own):
    blocks = to_y([own] * 4)
    mine = jnp.concatenate(blocks, axis=0)
    other = swap_core(mine)
    return jnp.concatenate([mine, other], axis=0)


def over_cores(partial):
    half = partial.shape[0] // 2
    other = swap_core(partial[half:])
    return wide_sum([partial[:half], other]).astype(jnp.bfloat16)


def over_group(mine, extra):
    n = mine.shape[0] // 4
    tiles = [mine[i * n : (i + 1) * n] for i in (0, 2, 1, 3)]
    if extra is None:
        return wide_sum(to_y(tiles))
    total = wide_sum(to_y([jnp.concatenate([t, extra]) for t in tiles]))
    return total[:n], total[n:]


def scatter_z(part):
    n_z = lax.axis_size("z")
    part = part.reshape(n_z, part.shape[0] // n_z, part.shape[1])
    part = lax.all_to_all(part, "z", 0, 0, tiled=True)
    return wide_sum([part[i] for i in range(n_z)]).astype(jnp.bfloat16)


def gather_z(own):
    n_z = lax.axis_size("z")
    z = lax.axis_index("z")
    half = own.shape[0] // 2
    whole = jnp.zeros((n_z, *own.shape), own.dtype)

    def put(whole, block, step, row):
        return lax.dynamic_update_slice(whole, block[None], (lax.rem(z + step + n_z, n_z), row, 0))

    whole = put(whole, own, 0, 0)
    low = high = own
    for k in range(1, n_z // 2):
        low, high = shift(low, "z", n_z, 1), shift(high, "z", n_z, n_z - 1)
        whole = put(put(whole, low, -k, 0), high, k, 0)
    low, high = shift(low[:half], "z", n_z, 1), shift(high[half:], "z", n_z, n_z - 1)
    whole = put(put(whole, low, -(n_z // 2), 0), high, n_z // 2, half)
    return whole


def block(patches, norm_gain, norm_bias, up_weight, up_bias, down_weight, down_bias, cotangent):
    local_rows, width = patches.shape
    total_rows = local_rows * math.prod(lax.axis_size(a) for a in AXES)
    scaling = 1.0 / math.sqrt(total_rows)
    c, xh = lax.axis_index("c"), lax.axis_index("xh")
    half_h = up_weight.shape[1] // 2
    half_d = width // 2

    def turned(array):
        return jnp.where(xh == 0, array, jnp.concatenate([array[:, half_d:], array[:, :half_d]], axis=1))

    def by_core(first, second):
        return jnp.where(c == 0, first, second)

    bias_own = by_core(up_bias[:half_h], up_bias[half_h:])[None]
    bias_flip = flip_x(bias_own, 1, 0)
    bias_row = jnp.concatenate([bias_own, bias_flip], axis=1)
    up_own = by_core(up_weight[:, :half_h], up_weight[:, half_h:])
    up = square(from_x(up_own))
    down_own = by_core(down_weight[:half_h], down_weight[half_h:]).T
    down = square(from_x(down_own))

    wide_patches = patches.astype(jnp.float32)
    centred = wide_patches - jnp.mean(wide_patches, axis=1, keepdims=True)
    inverse_spread = lax.rsqrt(jnp.mean(centred * centred, axis=1, keepdims=True) + EPSILON)
    standard = centred * inverse_spread
    normed = (standard * norm_gain + norm_bias).astype(jnp.bfloat16)

    normed_rows = tokens_of_group(turned(normed))
    upstream = tokens_of_group(turned(cotangent))

    preact = dot(normed_rows, up, 1, 0) + bias_row
    activated, slope = gelu_value(preact).astype(jnp.bfloat16), gelu_slope(preact)
    activated, slope = lax.optimization_barrier((activated, slope))
    down_full = dot(upstream, activated, 0, 0).astype(jnp.bfloat16)
    down_grad = scatter_z(sum_to_x(quarters(down_full)))
    slope = (dot(upstream, down, 1, 0) * slope).astype(jnp.bfloat16)
    up_full = dot(normed_rows, slope, 0, 0).astype(jnp.bfloat16)
    up_grad = scatter_z(sum_to_x(quarters(up_full)))
    back_rows = dot(slope, up, 1, 1).astype(jnp.bfloat16)
    back_rows = over_cores(back_rows)
    out_rows = dot(activated, down, 1, 1).astype(jnp.bfloat16)
    out_rows = over_cores(out_rows)
    normed_back = turned(over_group(back_rows, None))

    norm_part = jnp.stack([jnp.sum(normed_back * standard, axis=0), jnp.sum(normed_back, axis=0)])
    norm_part = jnp.pad(norm_part, ((0, 14), (0, 0))).astype(jnp.bfloat16)
    projected, norm_part = over_group(out_rows, norm_part)
    output = turned(projected) + down_bias + wide_patches

    norm_part = norm_part[:2].reshape(-1, 128)
    bias_sum = dot(jnp.ones((8, slope.shape[0]), jnp.bfloat16), slope, 1, 0)[0].reshape(-1, 128)
    n = bias_sum.shape[0] // 2
    stay = jnp.concatenate([norm_part, bias_sum[:n]])
    move = jnp.concatenate([norm_part, bias_sum[n:]])
    small = wide_sum(to_x([stay, move, move, stay]))
    rows = -(-small.size // half_h // 16) * 16
    small = jnp.pad(small.ravel(), (0, rows * half_h - small.size)).reshape(rows, half_h)
    whole = gather_z(jnp.concatenate([up_grad, down_grad, small.astype(jnp.bfloat16)]))
    other = swap_core(whole)
    n = up_grad.shape[0]
    small, small_other = (jnp.sum(a[:, -rows:].astype(jnp.float32), axis=0).ravel() * scaling for a in (whole, other))
    norm_grad = (small[: 2 * width] + small_other[: 2 * width]).reshape(2, width)
    bias_own, bias_other = (a[2 * width : 2 * width + half_h] for a in (small, small_other))
    bias_grad = by_core(jnp.concatenate([bias_own, bias_other]), jnp.concatenate([bias_other, bias_own]))

    up_part, up_away = (a[:, :n].reshape(-1, half_h) for a in (whole, other))
    up_grad = by_core(
        jnp.concatenate([up_part, up_away], axis=1), jnp.concatenate([up_away, up_part], axis=1)
    )
    up_grad = up_grad.astype(jnp.float32) * scaling
    down_part, down_away = (
        a[:, n : 2 * n].reshape(-1, half_h).T.astype(jnp.float32) * scaling for a in (whole, other)
    )
    down_grad = jnp.zeros((2 * half_h, half_d), jnp.float32)
    down_grad = lax.dynamic_update_slice(down_grad, down_part, (c * half_h, 0))
    down_grad = lax.dynamic_update_slice(down_grad, down_away, ((1 - c) * half_h, 0))

    scaled = normed_back * norm_gain
    back = inverse_spread * (
        scaled
        - jnp.mean(scaled, axis=1, keepdims=True)
        - standard * jnp.mean(scaled * standard, axis=1, keepdims=True)
    )
    patch_grad = back + cotangent.astype(jnp.float32)

    return output, patch_grad, up_grad, down_grad, bias_grad, norm_grad


def solution(mesh):
    split = Mesh(mesh.devices.reshape(8, 2, 2, 4, 2), AXES)
    tokens = P(AXES, None)
    rows = ("xl", "y")
    return jax.shard_map(
        block,
        mesh=split,
        in_specs=(tokens, P(), P(), P("xh", rows), P(rows), P(rows, "xh"), P(), tokens),
        out_specs=(tokens, tokens, P("xh", rows), P(rows, "xh"), P(rows), P()),
        check_vma=False,
    )
```

```python
import math

import jax
import jax.numpy as jnp
from jax import lax
from jax.sharding import Mesh
from jax.sharding import PartitionSpec as P


AXES = ("z", "c", "xl", "y", "xh")
X = ("xl", "xh")

EPSILON = 1e-06
GELU_ROOT = 0.7978845608028654
GELU_CUBIC = 0.044715


def gelu_value(value):
    inner = jnp.tanh(GELU_ROOT * (value + GELU_CUBIC * value * value * value))
    return 0.5 * value * (1.0 + inner)


def gelu_slope(value):
    inner = jnp.tanh(GELU_ROOT * (value + GELU_CUBIC * value * value * value))
    return 0.5 * (1.0 + inner) + 0.5 * value * (1.0 - inner * inner) * GELU_ROOT * (
        1.0 + 3.0 * GELU_CUBIC * value * value
    )


def dot(left, right, lc, rc):
    return lax.dot_general(
        left, right, (((lc,), (rc,)), ((), ())), preferred_element_type=jnp.float32
    )


def shift(array, axis, size, k):
    return lax.ppermute(array, axis, [(i, (i + k) % size) for i in range(size)])


def flip_x(array, l, h):
    return lax.ppermute(array, X, [(i, i ^ (2 * l + h)) for i in range(4)])


def swap_core(array):
    return lax.ppermute(array, "c", [(0, 1), (1, 0)])


def to_x(tiles):
    return [tiles[0], flip_x(tiles[1], 1, 0), flip_x(tiles[2], 1, 1), flip_x(tiles[3], 0, 1)]


def from_x(own):
    side, other = flip_x(own, 1, 0), flip_x(own, 1, 1)
    half = own.shape[0] // 2
    far = jnp.concatenate([flip_x(other[:half], 1, 0), flip_x(side[half:], 1, 1)])
    return [own, side, other, far]


def sum_to_x(tiles):
    own, side, other, far = tiles
    half = own.shape[0] // 2
    for_other, for_side = flip_x(far[:half], 1, 0), flip_x(far[half:], 1, 1)
    side = jnp.concatenate([side[:half], wide_sum([side[half:], for_side]).astype(jnp.bfloat16)])
    other = jnp.concatenate([wide_sum([other[:half], for_other]).astype(jnp.bfloat16), other[half:]])
    side, other = flip_x(side, 1, 0), flip_x(other, 1, 1)
    return wide_sum([own, side, other]).astype(jnp.bfloat16)


def to_y(tiles):
    return [
        tiles[0],
        shift(tiles[1], "y", 4, 1),
        shift(tiles[2], "y", 4, 3),
        shift(tiles[3], "y", 4, 2),
    ]


def square(tiles):
    top = jnp.concatenate([tiles[0], tiles[1]], axis=1)
    low = jnp.concatenate([tiles[3], tiles[2]], axis=1)
    return jnp.concatenate([top, low], axis=0)


def quarters(full):
    r, k = full.shape[0] // 2, full.shape[1] // 2
    return [full[:r, :k], full[:r, k:], full[r:, k:], full[r:, :k]]


def wide_sum(tiles):
    return sum(t.astype(jnp.float32) for t in tiles)


def tokens_of_group(own):
    blocks = to_y([own] * 4)
    mine = jnp.concatenate(blocks, axis=0)
    other = swap_core(mine)
    return jnp.concatenate([mine, other], axis=0)


def over_cores(partial):
    half = partial.shape[0] // 2
    other = swap_core(partial[half:])
    return wide_sum([partial[:half], other]).astype(jnp.bfloat16)


def over_group(mine, extra):
    n = mine.shape[0] // 4
    tiles = [mine[i * n : (i + 1) * n] for i in (0, 2, 1, 3)]
    if extra is None:
        return wide_sum(to_y(tiles))
    total = wide_sum(to_y([jnp.concatenate([t, extra]) for t in tiles]))
    return total[:n], total[n:]


def scatter_z(part):
    n_z = lax.axis_size("z")
    part = part.reshape(n_z, part.shape[0] // n_z, part.shape[1])
    part = lax.all_to_all(part, "z", 0, 0, tiled=True)
    return wide_sum([part[i] for i in range(n_z)]).astype(jnp.bfloat16)


def gather_z(own):
    n_z = lax.axis_size("z")
    z = lax.axis_index("z")
    half = own.shape[0] // 2
    whole = jnp.zeros((n_z, *own.shape), own.dtype)

    def put(whole, block, step, row):
        return lax.dynamic_update_slice(whole, block[None], (lax.rem(z + step + n_z, n_z), row, 0))

    whole = put(whole, own, 0, 0)
    low = high = own
    for k in range(1, n_z // 2):
        low, high = shift(low, "z", n_z, 1), shift(high, "z", n_z, n_z - 1)
        whole = put(put(whole, low, -k, 0), high, k, 0)
    low, high = shift(low[:half], "z", n_z, 1), shift(high[half:], "z", n_z, n_z - 1)
    whole = put(put(whole, low, -(n_z // 2), 0), high, n_z // 2, half)
    return whole


def block(patches, norm_gain, norm_bias, up_weight, up_bias, down_weight, down_bias, cotangent):
    local_rows, width = patches.shape
    total_rows = local_rows * math.prod(lax.axis_size(a) for a in AXES)
    scaling = 1.0 / math.sqrt(total_rows)
    c, xh = lax.axis_index("c"), lax.axis_index("xh")
    half_h = up_weight.shape[1] // 2
    half_d = width // 2

    def turned(array):
        return jnp.where(xh == 0, array, jnp.concatenate([array[:, half_d:], array[:, :half_d]], axis=1))

    def by_core(first, second):
        return jnp.where(c == 0, first, second)

    bias_own = by_core(up_bias[:half_h], up_bias[half_h:])[None]
    bias_flip = flip_x(bias_own, 1, 0)
    bias_row = jnp.concatenate([bias_own, bias_flip], axis=1)
    up_own = by_core(up_weight[:, :half_h], up_weight[:, half_h:])
    up = square(from_x(up_own))
    down_own = by_core(down_weight[:half_h], down_weight[half_h:]).T
    down = square(from_x(down_own))

    wide_patches = patches.astype(jnp.float32)
    centred = wide_patches - jnp.mean(wide_patches, axis=1, keepdims=True)
    inverse_spread = lax.rsqrt(jnp.mean(centred * centred, axis=1, keepdims=True) + EPSILON)
    standard = centred * inverse_spread
    normed = (standard * norm_gain + norm_bias).astype(jnp.bfloat16)

    normed_rows = tokens_of_group(turned(normed))
    upstream = tokens_of_group(turned(cotangent))

    preact = dot(normed_rows, up, 1, 0) + bias_row
    activated, slope = gelu_value(preact).astype(jnp.bfloat16), gelu_slope(preact)
    activated, slope = lax.optimization_barrier((activated, slope))
    down_full = dot(upstream, activated, 0, 0).astype(jnp.bfloat16)
    down_grad = scatter_z(sum_to_x(quarters(down_full)))
    slope = (dot(upstream, down, 1, 0) * slope).astype(jnp.bfloat16)
    up_full = dot(normed_rows, slope, 0, 0).astype(jnp.bfloat16)
    up_grad = scatter_z(sum_to_x(quarters(up_full)))
    back_rows = dot(slope, up, 1, 1).astype(jnp.bfloat16)
    back_rows = over_cores(back_rows)
    out_rows = dot(activated, down, 1, 1).astype(jnp.bfloat16)
    out_rows = over_cores(out_rows)
    normed_back = turned(over_group(back_rows, None))

    norm_part = jnp.stack([jnp.sum(normed_back * standard, axis=0), jnp.sum(normed_back, axis=0)])
    norm_part = jnp.pad(norm_part, ((0, 14), (0, 0))).astype(jnp.bfloat16)
    projected, norm_part = over_group(out_rows, norm_part)
    output = turned(projected) + down_bias + wide_patches

    norm_part = norm_part[:2].reshape(-1, 128)
    bias_sum = dot(jnp.ones((8, slope.shape[0]), jnp.bfloat16), slope, 1, 0)[0].reshape(-1, 128)
    n = bias_sum.shape[0] // 2
    stay = jnp.concatenate([norm_part, bias_sum[:n]])
    move = jnp.concatenate([norm_part, bias_sum[n:]])
    small = wide_sum(to_x([stay, move, move, stay]))
    rows = -(-small.size // half_h // 16) * 16
    small = jnp.pad(small.ravel(), (0, rows * half_h - small.size)).reshape(rows, half_h)
    whole = gather_z(jnp.concatenate([up_grad, down_grad, small.astype(jnp.bfloat16)]))
    other = swap_core(whole)
    n = up_grad.shape[0]
    small, small_other = (jnp.sum(a[:, -rows:].astype(jnp.float32), axis=0).ravel() * scaling for a in (whole, other))
    norm_grad = (small[: 2 * width] + small_other[: 2 * width]).reshape(2, width)
    bias_own, bias_other = (a[2 * width : 2 * width + half_h] for a in (small, small_other))
    bias_grad = by_core(jnp.concatenate([bias_own, bias_other]), jnp.concatenate([bias_other, bias_own]))

    up_part, up_away = (a[:, :n].reshape(-1, half_h) for a in (whole, other))
    up_grad = by_core(
        jnp.concatenate([up_part, up_away], axis=1), jnp.concatenate([up_away, up_part], axis=1)
    )
    up_grad = up_grad.astype(jnp.float32) * scaling
    down_part, down_away = (a[:, n : 2 * n].reshape(-1, half_h) for a in (whole, other))
    down_grad = by_core(
        jnp.concatenate([down_part, down_away], axis=1), jnp.concatenate([down_away, down_part], axis=1)
    )
    down_grad = (down_grad.astype(jnp.float32) * scaling).T

    scaled = normed_back * norm_gain
    back = inverse_spread * (
        scaled
        - jnp.mean(scaled, axis=1, keepdims=True)
        - standard * jnp.mean(scaled * standard, axis=1, keepdims=True)
    )
    patch_grad = back + cotangent.astype(jnp.float32)

    return output, patch_grad, up_grad, down_grad, bias_grad, norm_grad


def solution(mesh):
    split = Mesh(mesh.devices.reshape(8, 2, 2, 4, 2), AXES)
    tokens = P(AXES, None)
    rows = ("xl", "y")
    return jax.shard_map(
        block,
        mesh=split,
        in_specs=(tokens, P(), P(), P("xh", rows), P(rows), P(rows, "xh"), P(), tokens),
        out_specs=(tokens, tokens, P("xh", rows), P(rows, "xh"), P(rows), P()),
        check_vma=False,
    )
```

```python
import math

import jax
import jax.numpy as jnp
from jax import lax
from jax.sharding import Mesh
from jax.sharding import PartitionSpec as P


AXES = ("z", "c", "xl", "y", "xh")
X = ("xl", "xh")

EPSILON = 1e-06
GELU_ROOT = 0.7978845608028654
GELU_CUBIC = 0.044715


def gelu_value(value):
    inner = jnp.tanh(GELU_ROOT * (value + GELU_CUBIC * value * value * value))
    return 0.5 * value * (1.0 + inner)


def gelu_slope(value):
    inner = jnp.tanh(GELU_ROOT * (value + GELU_CUBIC * value * value * value))
    return 0.5 * (1.0 + inner) + 0.5 * value * (1.0 - inner * inner) * GELU_ROOT * (
        1.0 + 3.0 * GELU_CUBIC * value * value
    )


def dot(left, right, lc, rc):
    return lax.dot_general(
        left, right, (((lc,), (rc,)), ((), ())), preferred_element_type=jnp.float32
    )


def shift(array, axis, size, k):
    return lax.ppermute(array, axis, [(i, (i + k) % size) for i in range(size)])


def flip_x(array, l, h):
    return lax.ppermute(array, X, [(i, i ^ (2 * l + h)) for i in range(4)])


def swap_core(array):
    return lax.ppermute(array, "c", [(0, 1), (1, 0)])


def to_x(tiles):
    return [tiles[0], flip_x(tiles[1], 1, 0), flip_x(tiles[2], 1, 1), flip_x(tiles[3], 0, 1)]


def from_x(own):
    side, other = flip_x(own, 1, 0), flip_x(own, 1, 1)
    half = own.shape[0] // 2
    far = jnp.concatenate([flip_x(other[:half], 1, 0), flip_x(side[half:], 1, 1)])
    return [own, side, other, far]


def sum_to_x(tiles):
    own, side, other, far = tiles
    half = own.shape[0] // 2
    for_other, for_side = flip_x(far[:half], 1, 0), flip_x(far[half:], 1, 1)
    side = jnp.concatenate([side[:half], wide_sum([side[half:], for_side]).astype(jnp.bfloat16)])
    other = jnp.concatenate([wide_sum([other[:half], for_other]).astype(jnp.bfloat16), other[half:]])
    side, other = flip_x(side, 1, 0), flip_x(other, 1, 1)
    return wide_sum([own, side, other]).astype(jnp.bfloat16)


def to_y(tiles):
    return [
        tiles[0],
        shift(tiles[1], "y", 4, 1),
        shift(tiles[2], "y", 4, 3),
        shift(tiles[3], "y", 4, 2),
    ]


def square(tiles):
    top = jnp.concatenate([tiles[0], tiles[1]], axis=1)
    low = jnp.concatenate([tiles[3], tiles[2]], axis=1)
    return jnp.concatenate([top, low], axis=0)


def quarters(full):
    r, k = full.shape[0] // 2, full.shape[1] // 2
    return [full[:r, :k], full[:r, k:], full[r:, k:], full[r:, :k]]


def wide_sum(tiles):
    return sum(t.astype(jnp.float32) for t in tiles)


def tokens_of_group(own):
    blocks = to_y([own] * 4)
    mine = jnp.concatenate(blocks, axis=0)
    other = swap_core(mine)
    return jnp.concatenate([mine, other], axis=0)


def tokens_to_owner(partial, extra):
    half = partial.shape[0] // 2
    n = half // 4
    send = [partial[half:]] + ([extra] if extra is not None else [])
    other = swap_core(jnp.concatenate(send) if len(send) > 1 else send[0])
    mine = wide_sum([partial[:half], other[:half]]).astype(jnp.bfloat16)
    tiles = [mine[i * n : (i + 1) * n] for i in (0, 2, 1, 3)]
    if extra is None:
        return wide_sum(to_y(tiles))
    extra = wide_sum([extra, other[half:]]).astype(jnp.bfloat16)
    total = wide_sum(to_y([jnp.concatenate([t, extra]) for t in tiles]))
    return total[:n], total[n:]


def scatter_z(part):
    n_z = lax.axis_size("z")
    part = part.reshape(n_z, part.shape[0] // n_z, part.shape[1])
    part = lax.all_to_all(part, "z", 0, 0, tiled=True)
    return wide_sum([part[i] for i in range(n_z)]).astype(jnp.bfloat16)


def gather_z(own):
    n_z = lax.axis_size("z")
    z = lax.axis_index("z")
    half = own.shape[0] // 2
    whole = jnp.zeros((n_z, *own.shape), own.dtype)

    def put(whole, block, step, row):
        return lax.dynamic_update_slice(whole, block[None], (lax.rem(z + step + n_z, n_z), row, 0))

    whole = put(whole, own, 0, 0)
    low, high = shift(own, "z", n_z, 2), shift(own, "z", n_z, n_z - 2)
    next_low, next_high = shift(own, "z", n_z, 1), shift(own, "z", n_z, n_z - 1)
    whole = put(put(whole, low, -2, 0), high, 2, 0)
    whole = put(put(whole, next_low, -1, 0), next_high, 1, 0)
    far_low, far_high = shift(low[:half], "z", n_z, 2), shift(high[half:], "z", n_z, n_z - 2)
    low, high = shift(low, "z", n_z, 1), shift(high, "z", n_z, n_z - 1)
    whole = put(put(whole, low, -3, 0), high, 3, 0)
    return put(put(whole, far_low, -4, 0), far_high, 4, half)


def block(patches, norm_gain, norm_bias, up_weight, up_bias, down_weight, down_bias, cotangent):
    local_rows, width = patches.shape
    total_rows = local_rows * math.prod(lax.axis_size(a) for a in AXES)
    scaling = 1.0 / math.sqrt(total_rows)
    c, xh = lax.axis_index("c"), lax.axis_index("xh")
    half_h = up_weight.shape[1] // 2
    half_d = width // 2

    def turned(array):
        return jnp.where(xh == 0, array, jnp.concatenate([array[:, half_d:], array[:, :half_d]], axis=1))

    def by_core(first, second):
        return jnp.where(c == 0, first, second)

    bias_own = by_core(up_bias[:half_h], up_bias[half_h:])[None]
    bias_flip = flip_x(bias_own, 1, 0)
    bias_row = jnp.concatenate([bias_own, bias_flip], axis=1)
    up_own = by_core(up_weight[:, :half_h], up_weight[:, half_h:])
    up = square(from_x(up_own))
    down_own = by_core(down_weight[:half_h], down_weight[half_h:]).T
    down = square(from_x(down_own))

    wide_patches = patches.astype(jnp.float32)
    centred = wide_patches - jnp.mean(wide_patches, axis=1, keepdims=True)
    inverse_spread = lax.rsqrt(jnp.mean(centred * centred, axis=1, keepdims=True) + EPSILON)
    standard = centred * inverse_spread
    normed = (standard * norm_gain + norm_bias).astype(jnp.bfloat16)

    normed_rows = tokens_of_group(turned(normed))
    upstream = tokens_of_group(turned(cotangent))

    preact = dot(normed_rows, up, 1, 0) + bias_row
    activated, slope = gelu_value(preact).astype(jnp.bfloat16), gelu_slope(preact)
    activated, slope = lax.optimization_barrier((activated, slope))
    down_full = dot(upstream, activated, 0, 0).astype(jnp.bfloat16)
    down_grad = scatter_z(sum_to_x(quarters(down_full)))
    slope = (dot(upstream, down, 1, 0) * slope).astype(jnp.bfloat16)
    up_full = dot(normed_rows, slope, 0, 0).astype(jnp.bfloat16)
    up_grad = scatter_z(sum_to_x(quarters(up_full)))
    back_rows = dot(slope, up, 1, 1).astype(jnp.bfloat16)
    normed_back = turned(tokens_to_owner(back_rows, None))

    norm_part = jnp.stack([jnp.sum(normed_back * standard, axis=0), jnp.sum(normed_back, axis=0)])
    norm_part = jnp.pad(norm_part, ((0, 14), (0, 0))).astype(jnp.bfloat16)
    out_rows = dot(activated, down, 1, 1).astype(jnp.bfloat16)
    projected, norm_part = tokens_to_owner(out_rows, norm_part)
    output = turned(projected) + down_bias + wide_patches

    norm_part = norm_part[:2].reshape(-1, 128)
    bias_sum = dot(jnp.ones((8, slope.shape[0]), jnp.bfloat16), slope, 1, 0)[0].reshape(-1, 128)
    n = bias_sum.shape[0] // 2
    stay = jnp.concatenate([norm_part, bias_sum[:n]])
    move = jnp.concatenate([norm_part, bias_sum[n:]])
    small = wide_sum(to_x([stay, move, move, stay]))
    rows = -(-small.size // half_h // 16) * 16
    small = jnp.pad(small.ravel(), (0, rows * half_h - small.size)).reshape(rows, half_h)
    whole = gather_z(jnp.concatenate([up_grad, down_grad, small.astype(jnp.bfloat16)]))
    other = swap_core(whole)
    n = up_grad.shape[0]
    small = jnp.sum(whole[:, -rows:].astype(jnp.float32), axis=0).ravel() * scaling
    norm_grad = small[: 2 * width].reshape(2, width)
    bias_own = small[2 * width : 2 * width + half_h]
    bias_other = jnp.sum(other[:, -rows:].astype(jnp.float32), axis=0).ravel() * scaling
    bias_other = bias_other[2 * width : 2 * width + half_h]
    bias_grad = by_core(jnp.concatenate([bias_own, bias_other]), jnp.concatenate([bias_other, bias_own]))

    def both_cores(at):
        part, away = (a[:, at : at + n].reshape(-1, half_h) for a in (whole, other))
        full = by_core(jnp.concatenate([part, away], axis=1), jnp.concatenate([away, part], axis=1))
        return full.astype(jnp.float32) * scaling

    scaled = normed_back * norm_gain
    back = inverse_spread * (
        scaled
        - jnp.mean(scaled, axis=1, keepdims=True)
        - standard * jnp.mean(scaled * standard, axis=1, keepdims=True)
    )
    patch_grad = back + cotangent.astype(jnp.float32)

    return output, patch_grad, both_cores(0), both_cores(n).T, bias_grad, norm_grad


def solution(mesh):
    split = Mesh(mesh.devices.reshape(8, 2, 2, 4, 2), AXES)
    tokens = P(AXES, None)
    rows = ("xl", "y")
    return jax.shard_map(
        block,
        mesh=split,
        in_specs=(tokens, P(), P(), P("xh", rows), P(rows), P(rows, "xh"), P(), tokens),
        out_specs=(tokens, tokens, P("xh", rows), P(rows, "xh"), P(rows), P()),
        check_vma=False,
    )
```

```python
import math

import jax
import jax.numpy as jnp
from jax import lax
from jax.sharding import Mesh
from jax.sharding import PartitionSpec as P


AXES = ("z", "c", "xl", "y", "xh")
X = ("xl", "xh")

EPSILON = 1e-06
GELU_ROOT = 0.7978845608028654
GELU_CUBIC = 0.044715


def gelu_value(value):
    inner = jnp.tanh(GELU_ROOT * (value + GELU_CUBIC * value * value * value))
    return 0.5 * value * (1.0 + inner)


def gelu_slope(value):
    inner = jnp.tanh(GELU_ROOT * (value + GELU_CUBIC * value * value * value))
    return 0.5 * (1.0 + inner) + 0.5 * value * (1.0 - inner * inner) * GELU_ROOT * (
        1.0 + 3.0 * GELU_CUBIC * value * value
    )


def dot(left, right, lc, rc):
    return lax.dot_general(
        left, right, (((lc,), (rc,)), ((), ())), preferred_element_type=jnp.float32
    )


def shift(array, axis, size, k):
    return lax.ppermute(array, axis, [(i, (i + k) % size) for i in range(size)])


def flip_x(array, l, h):
    return lax.ppermute(array, X, [(i, i ^ (2 * l + h)) for i in range(4)])


def swap_core(array):
    return lax.ppermute(array, "c", [(0, 1), (1, 0)])


def to_x(tiles):
    return [tiles[0], flip_x(tiles[1], 1, 0), flip_x(tiles[2], 1, 1), flip_x(tiles[3], 0, 1)]


def from_x(own):
    side, other = flip_x(own, 1, 0), flip_x(own, 1, 1)
    half = own.shape[0] // 2
    far = jnp.concatenate([flip_x(other[:half], 1, 0), flip_x(side[half:], 1, 1)])
    return [own, side, other, far]


def sum_to_x(tiles):
    own, side, other, far = tiles
    half = own.shape[0] // 2
    for_other, for_side = flip_x(far[:half], 1, 0), flip_x(far[half:], 1, 1)
    side = jnp.concatenate([side[:half], wide_sum([side[half:], for_side]).astype(jnp.bfloat16)])
    other = jnp.concatenate([wide_sum([other[:half], for_other]).astype(jnp.bfloat16), other[half:]])
    side, other = flip_x(side, 1, 0), flip_x(other, 1, 1)
    return wide_sum([own, side, other]).astype(jnp.bfloat16)


def to_y(tiles):
    return [
        tiles[0],
        shift(tiles[1], "y", 4, 1),
        shift(tiles[2], "y", 4, 3),
        shift(tiles[3], "y", 4, 2),
    ]


def square(tiles):
    top = jnp.concatenate([tiles[0], tiles[1]], axis=1)
    low = jnp.concatenate([tiles[3], tiles[2]], axis=1)
    return jnp.concatenate([top, low], axis=0)


def quarters(full):
    r, k = full.shape[0] // 2, full.shape[1] // 2
    return [full[:r, :k], full[:r, k:], full[r:, k:], full[r:, :k]]


def wide_sum(tiles):
    return sum(t.astype(jnp.float32) for t in tiles)


def tokens_of_group(own):
    blocks = to_y([own] * 4)
    mine = jnp.concatenate(blocks, axis=0)
    other = swap_core(mine)
    return jnp.concatenate([mine, other], axis=0)


def tokens_to_owner(partial, extra):
    half = partial.shape[0] // 2
    n = half // 4
    send = [partial[half:]] + ([extra] if extra is not None else [])
    other = swap_core(jnp.concatenate(send) if len(send) > 1 else send[0])
    mine = wide_sum([partial[:half], other[:half]]).astype(jnp.bfloat16)
    tiles = [mine[i * n : (i + 1) * n] for i in (0, 2, 1, 3)]
    if extra is None:
        return wide_sum(to_y(tiles))
    extra = wide_sum([extra, other[half:]]).astype(jnp.bfloat16)
    tiles = to_y([jnp.concatenate([t, extra]) for t in tiles])
    small = lax.optimization_barrier([t[n : n + 8] for t in tiles])
    return wide_sum([t[:n] for t in tiles]), wide_sum(small)


def scatter_z(part):
    n_z = lax.axis_size("z")
    part = part.reshape(n_z, part.shape[0] // n_z, part.shape[1])
    part = lax.all_to_all(part, "z", 0, 0, tiled=True)
    return wide_sum([part[i] for i in range(n_z)]).astype(jnp.bfloat16)


def gather_z(own):
    n_z = lax.axis_size("z")
    z = lax.axis_index("z")
    half = own.shape[0] // 2
    whole = jnp.zeros((n_z, *own.shape), own.dtype)

    def put(whole, block, step, row):
        return lax.dynamic_update_slice(whole, block[None], (lax.rem(z + step + n_z, n_z), row, 0))

    whole = put(whole, own, 0, 0)
    low, high = shift(own, "z", n_z, 2), shift(own, "z", n_z, n_z - 2)
    next_low, next_high = shift(own, "z", n_z, 1), shift(own, "z", n_z, n_z - 1)
    whole = put(put(whole, low, -2, 0), high, 2, 0)
    whole = put(put(whole, next_low, -1, 0), next_high, 1, 0)
    far_low, far_high = shift(low[:half], "z", n_z, 2), shift(high[half:], "z", n_z, n_z - 2)
    low, high = shift(low, "z", n_z, 1), shift(high, "z", n_z, n_z - 1)
    whole = put(put(whole, low, -3, 0), high, 3, 0)
    return put(put(whole, far_low, -4, 0), far_high, 4, half)


def block(patches, norm_gain, norm_bias, up_weight, up_bias, down_weight, down_bias, cotangent):
    local_rows, width = patches.shape
    total_rows = local_rows * math.prod(lax.axis_size(a) for a in AXES)
    scaling = 1.0 / math.sqrt(total_rows)
    c, xh = lax.axis_index("c"), lax.axis_index("xh")
    half_h = up_weight.shape[1] // 2
    half_d = width // 2

    def turned(array):
        return jnp.where(xh == 0, array, jnp.concatenate([array[:, half_d:], array[:, :half_d]], axis=1))

    def by_core(first, second):
        return jnp.where(c == 0, first, second)

    bias_own = by_core(up_bias[:half_h], up_bias[half_h:])[None]
    bias_flip = flip_x(bias_own, 1, 0)
    bias_row = jnp.concatenate([bias_own, bias_flip], axis=1)
    up_own = by_core(up_weight[:, :half_h], up_weight[:, half_h:])
    up = square(from_x(up_own))
    down_own = by_core(down_weight[:half_h], down_weight[half_h:]).T
    down = square(from_x(down_own))

    wide_patches = patches.astype(jnp.float32)
    centred = wide_patches - jnp.mean(wide_patches, axis=1, keepdims=True)
    inverse_spread = lax.rsqrt(jnp.mean(centred * centred, axis=1, keepdims=True) + EPSILON)
    standard = centred * inverse_spread
    normed = (standard * norm_gain + norm_bias).astype(jnp.bfloat16)

    normed_rows = tokens_of_group(turned(normed))
    upstream = tokens_of_group(turned(cotangent))

    preact = dot(normed_rows, up, 1, 0) + bias_row
    activated, slope = gelu_value(preact).astype(jnp.bfloat16), gelu_slope(preact)
    activated, slope = lax.optimization_barrier((activated, slope))
    down_full = dot(upstream, activated, 0, 0).astype(jnp.bfloat16)
    down_grad = scatter_z(sum_to_x(quarters(down_full)))
    slope = (dot(upstream, down, 1, 0) * slope).astype(jnp.bfloat16)
    up_full = dot(normed_rows, slope, 0, 0).astype(jnp.bfloat16)
    up_grad = scatter_z(sum_to_x(quarters(up_full)))
    back_rows = dot(slope, up, 1, 1).astype(jnp.bfloat16)
    normed_back = turned(tokens_to_owner(back_rows, None))

    norm_part = jnp.stack([jnp.sum(normed_back * standard, axis=0), jnp.sum(normed_back, axis=0)])
    norm_part = jnp.pad(norm_part, ((0, 14), (0, 0))).astype(jnp.bfloat16)
    out_rows = dot(activated, down, 1, 1).astype(jnp.bfloat16)
    projected, norm_part = tokens_to_owner(out_rows, norm_part)
    output = turned(projected) + down_bias + wide_patches

    norm_part = norm_part[:2].reshape(-1, 128)
    bias_sum = dot(jnp.ones((8, slope.shape[0]), jnp.bfloat16), slope, 1, 0)[0].reshape(-1, 128)
    n = bias_sum.shape[0] // 2
    stay = jnp.concatenate([norm_part, bias_sum[:n]])
    move = jnp.concatenate([norm_part, bias_sum[n:]])
    small = wide_sum(to_x([stay, move, move, stay]))
    rows = -(-small.size // half_h // 16) * 16
    small = jnp.pad(small.ravel(), (0, rows * half_h - small.size)).reshape(rows, half_h)
    whole = gather_z(jnp.concatenate([up_grad, down_grad, small.astype(jnp.bfloat16)]))
    other = swap_core(whole)
    n = up_grad.shape[0]
    small = jnp.sum(whole[:, -rows:].astype(jnp.float32), axis=0).ravel() * scaling
    norm_grad = small[: 2 * width].reshape(2, width)
    bias_own = small[2 * width : 2 * width + half_h]
    bias_other = jnp.sum(other[:, -rows:].astype(jnp.float32), axis=0).ravel() * scaling
    bias_other = bias_other[2 * width : 2 * width + half_h]
    bias_grad = by_core(jnp.concatenate([bias_own, bias_other]), jnp.concatenate([bias_other, bias_own]))

    def both_cores(at):
        part, away = (a[:, at : at + n].reshape(-1, half_h) for a in (whole, other))
        full = by_core(jnp.concatenate([part, away], axis=1), jnp.concatenate([away, part], axis=1))
        return full.astype(jnp.float32) * scaling

    scaled = normed_back * norm_gain
    back = inverse_spread * (
        scaled
        - jnp.mean(scaled, axis=1, keepdims=True)
        - standard * jnp.mean(scaled * standard, axis=1, keepdims=True)
    )
    patch_grad = back + cotangent.astype(jnp.float32)

    return output, patch_grad, both_cores(0), both_cores(n).T, bias_grad, norm_grad


def solution(mesh):
    split = Mesh(mesh.devices.reshape(8, 2, 2, 4, 2), AXES)
    tokens = P(AXES, None)
    rows = ("xl", "y")
    return jax.shard_map(
        block,
        mesh=split,
        in_specs=(tokens, P(), P(), P("xh", rows), P(rows), P(rows, "xh"), P(), tokens),
        out_specs=(tokens, tokens, P("xh", rows), P(rows, "xh"), P(rows), P()),
        check_vma=False,
    )
```
